128 devices in a mesh: segment: 2 (over core), mp: 64 (over x, y, z).
Axes of the slice: x: 4, y: 4, z: 4, core: 2. Of those that a mesh axis runs over, the one named last changes fastest.
Arguments:
- tokens: float32 [2, 128, 1024], P(None, 'mp'), may hold values from -6 to 6
- curvature: float32 [2, 128, 1024], P(None, 'mp'), may hold values from 0.05 to 0.5
- gains: float32 [2, 1024], P('segment'), may hold values from 0.1 to 1.9
- w_in: float32 [2, 1024, 65536], P('segment', None, 'mp'), may hold values from -0.1875 to 0.1875
- w_out: float32 [2, 65536, 1024], P('segment', 'mp'), may hold values from -0.0234375 to 0.0234375
- v_in: float32 [2, 1024, 65536], P('segment', None, 'mp'), may hold values from -0.1875 to 0.1875
- v_out: float32 [2, 65536, 1024], P('segment', 'mp'), may hold values from -0.0234375 to 0.0234375
Outputs:
- product_in: float32 [2, 1024, 65536], P('segment', None, 'mp')
- product_out: float32 [2, 65536, 1024], P('segment', 'mp')
The draws below stay inside these ranges and needn't reach their ends.
All inputs are finite; a program needn't handle non-finite values.
Results may differ from the reference program's by a relative error of at most 0.00011.
Values sent between devices are 32-bit elements; how exact they have to be, the bound alone decides.
No kernel may reach another device: no remote copies, remote signals or barrier semaphores. Data moves between devices by JAX's collectives and lax.ppermute only.
A program may use at most 128 MiB of HBM per device.

```python
import math
import jax
import jax.numpy as jnp
from jax import lax

D = 1024
FF = 65536
MB_ROWS = 128
MICRO = 2
LAYERS = 2


def block_scale(stream_key, extent, split, low, top_value):
    level = 1.0
    for dim, parts in split:
        steps = jax.random.uniform(jax.random.fold_in(jax.random.fold_in(stream_key, 6), dim), (parts,), jnp.float32, low / len(split), top_value / len(split))
        level = level * jnp.repeat(jnp.exp(steps), extent[dim] // parts).reshape((-1,) + (1,) * (len(extent) - 1 - dim))
    return level


def scatter_about(rng, extent, scale, limit, pieces=(), dtype=jnp.bfloat16):
    entries = scale * jax.random.normal(rng, extent, jnp.float32)
    if pieces:
        entries = entries * block_scale(rng, extent, pieces, -0.22, 0.18)
    return jnp.clip(entries, -limit, limit).astype(dtype)


def setup_inputs(seed: int = 0) -> dict:
    seeds = jax.random.split(jax.random.key(seed), 8)
    tokens = scatter_about(seeds[0], (MICRO, MB_ROWS, D), 1.0, 6.0, ((1, 64),), jnp.float32)
    curvature = jnp.clip(jnp.exp(math.log(0.5) - 2.3025851 * jax.random.uniform(seeds[1], (MICRO, MB_ROWS, D), jnp.float32) ** block_scale(seeds[1], (MICRO, MB_ROWS, D), ((1, 64),), -0.2, 0.2)), 0.05, 0.5)
    gains = jnp.clip(1.0 + 0.18 * jax.random.normal(seeds[2], (LAYERS, D), jnp.float32), 0.1, 1.9)
    w_in = scatter_about(seeds[3], (LAYERS, D, FF), D ** -0.5, 0.1875, ((0, 2), (2, 64)), jnp.float32)
    w_out = scatter_about(seeds[4], (LAYERS, FF, D), FF ** -0.5, 0.0234375, ((0, 2), (1, 64)), jnp.float32)
    v_in = scatter_about(seeds[5], (LAYERS, D, FF), D ** -0.5, 0.1875, ((0, 2), (2, 64)), jnp.float32)
    v_out = scatter_about(seeds[6], (LAYERS, FF, D), FF ** -0.5, 0.0234375, ((0, 2), (1, 64)), jnp.float32)
    return {"tokens": tokens, "curvature": curvature, "gains": gains, "w_in": w_in, "w_out": w_out, "v_in": v_in, "v_out": v_out}


eps = 1e-06
coeff = 0.7978845608028654

def mdot(a, b):
    return jnp.dot(a, b, precision=lax.Precision.HIGHEST, preferred_element_type=jnp.float32)

def gelu_pair(h):
    inner = coeff * (h + 0.044715 * h * h * h)
    tval = jnp.tanh(inner)
    act = 0.5 * h * (1.0 + tval)
    slope = 0.5 * (1.0 + tval) + 0.5 * h * (1.0 - tval * tval) * coeff * (1.0 + 3.0 * 0.044715 * h * h)
    return (act, slope)

def reference(tokens, curvature, gains, w_in, w_out, v_in, v_out):
    rows = tokens.reshape(MICRO * MB_ROWS, D)
    curv = curvature.reshape(MICRO * MB_ROWS, D)
    state = rows
    tangent = jnp.zeros_like(rows)
    saved = []
    for layer in range(LAYERS):
        gain = gains[layer]
        recip = lax.rsqrt(lax.optimization_barrier(jnp.mean(state * state, axis=-1, keepdims=True)) + eps)
        normed = state * recip * gain
        dnormed = gain * (tangent * recip - state * recip ** 3 * lax.optimization_barrier(jnp.mean(state * tangent, axis=-1, keepdims=True)))
        hidden = mdot(normed, w_in[layer])
        dhidden = mdot(dnormed, w_in[layer]) + mdot(normed, v_in[layer])
        act, slope = gelu_pair(hidden)
        dact = slope * dhidden
        saved.append((state, recip, normed, slope, act))
        tangent = tangent + mdot(dact, w_out[layer]) + mdot(act, v_out[layer])
        state = state + mdot(act, w_out[layer])
    cotan = curv * tangent
    grads_in = []
    grads_out = []
    for layer in range(LAYERS - 1, -1, -1):
        state, recip, normed, slope, act = saved[layer]
        grads_out.append(mdot(act.T, cotan))
        err = slope * mdot(cotan, w_out[layer].T)
        grads_in.append(mdot(normed.T, err))
        upart = gains[layer] * mdot(err, w_in[layer].T)
        cotan = cotan + upart * recip - state * recip ** 3 * lax.optimization_barrier(jnp.mean(state * upart, axis=-1, keepdims=True))
    grads_in = grads_in[::-1]
    grads_out = grads_out[::-1]
    return (jnp.stack(grads_in), jnp.stack(grads_out))
```

```python
import jax
import jax.numpy as jnp
from jax import lax
from jax.sharding import PartitionSpec as P

eps = 1e-06
coeff = 0.7978845608028654
HIGH = lax.Precision.HIGH


def dot(a, b, ca, cb):
    dims = (((ca,), (cb,)), ((), ()))
    return lax.dot_general(a, b, dims, precision=HIGH, preferred_element_type=jnp.float32)


def mdot(a, b):
    return dot(a, b, 1, 0)


def gelu_pair(h):
    inner = coeff * (h + 0.044715 * h * h * h)
    tval = jnp.tanh(inner)
    act = 0.5 * h * (1.0 + tval)
    slope = 0.5 * (1.0 + tval) + 0.5 * h * (1.0 - tval * tval) * coeff * (
        1.0 + 3.0 * 0.044715 * h * h
    )
    return act, slope


def mean(v):
    return jnp.mean(v, axis=-1, keepdims=True)


def across(v, source):
    return lax.ppermute(v, "segment", [(source, 1 - source)])


def gathered(piece):
    chips = lax.axis_size("mp")
    copies = jnp.broadcast_to(piece, (chips, *piece.shape))
    blocks = lax.all_to_all(copies, "mp", 0, 0, tiled=True)
    return blocks.reshape(chips * piece.shape[0], piece.shape[1])


def summed(half):
    chips = lax.axis_size("mp")
    blocks = half.reshape(chips, half.shape[0] // chips, half.shape[1])
    return jnp.sum(lax.all_to_all(blocks, "mp", 0, 0, tiled=True), axis=0)


def on_device(tokens, curvature, gains, w_in, w_out, v_in, v_out):
    core = lax.axis_index("segment")
    first = core == 0
    gain, wi, wo, vi, vo = gains, w_in[0], w_out[0], v_in[0], v_out[0]
    width = tokens.shape[2]
    x0 = lax.dynamic_index_in_dim(tokens, core, 0, keepdims=False)
    curv = lax.dynamic_index_in_dim(curvature, core, 0, keepdims=False)

    def reduced(total, source):
        half = total.shape[0] // 2
        own, other = total[:half], total[half:]
        came = across(other, source)
        return summed(jnp.where(core == source, own, came))

    def assembled(piece, target):
        own = gathered(piece)
        return jnp.concatenate([own, across(own, 1 - target)], axis=0)

    r0 = lax.rsqrt(mean(x0 * x0) + eps)
    n0 = assembled(x0 * r0, 0) * gain
    h = mdot(n0, wi)
    dh = mdot(n0, vi)
    a0, p0 = gelu_pair(h)
    da = p0 * dh
    out = mdot(a0, wo)
    dout = mdot(da, wo) + mdot(a0, vo)
    both = reduced(jnp.concatenate([out, dout], axis=1), 0)
    x1 = x0 + both[:, :width]
    dx1 = both[:, width:]

    r1 = lax.rsqrt(mean(x1 * x1) + eps)
    xr = x1 * r1
    dxr = dx1 * r1 - x1 * r1**3 * mean(x1 * dx1)
    both = assembled(jnp.concatenate([xr, dxr], axis=1), 1)
    n1 = both[:, :width] * gain
    dn1 = both[:, width:] * gain
    h = mdot(n1, wi)
    dh = mdot(dn1, wi) + mdot(n1, vi)
    a1, p1 = gelu_pair(h)
    da = p1 * dh
    dx2 = dx1 + reduced(mdot(da, wo) + mdot(a1, vo), 1)
    g2 = curv * dx2
    g2_all = assembled(g2, 1)

    e1 = p1 * dot(g2_all, wo, 1, 1)
    u = reduced(dot(e1, wi, 1, 1) * gain, 1)
    g1 = g2 + u * r1 - x1 * r1**3 * mean(x1 * u)
    g1_all = assembled(g1, 0)

    n = jnp.where(first, n0, n1)
    a = jnp.where(first, a0, a1)
    p = jnp.where(first, p0, p1)
    g = jnp.where(first, g1_all, g2_all)
    e = p * dot(g, wo, 1, 1)
    product_out = dot(a, g, 0, 0)
    product_in = dot(n, e, 0, 0)
    return product_in[None], product_out[None]


def solution(mesh):
    rows = P(None, "mp", None)
    layer_in = P("segment", None, "mp")
    layer_out = P("segment", "mp", None)
    return jax.shard_map(
        on_device,
        mesh=mesh,
        in_specs=(rows, rows, P("segment", None), layer_in, layer_out, layer_in, layer_out),
        out_specs=(layer_in, layer_out),
        check_vma=False,
    )
```

```python
import functools

import jax
import jax.numpy as jnp
from jax import lax
from jax.experimental import pallas as pl
from jax.experimental.pallas import tpu as pltpu
from jax.sharding import PartitionSpec as P

eps = 1e-06
coeff = 0.7978845608028654
f32 = jnp.float32
bf16 = jnp.bfloat16
UNITS = 256
MIB = 1 << 20


def gelu_pair(h):
    inner = coeff * (h + 0.044715 * h * h * h)
    tval = jnp.tanh(inner)
    act = 0.5 * h * (1.0 + tval)
    slope = 0.5 * (1.0 + tval) + 0.5 * h * (1.0 - tval * tval) * coeff * (
        1.0 + 3.0 * 0.044715 * h * h
    )
    return act, slope


def mean(v):
    return jnp.mean(v, axis=-1, keepdims=True)


def parts(v):
    high = v.astype(bf16)
    return high, (v - high.astype(f32)).astype(bf16)


def dot3(a, b, ca=1, cb=0):
    dims = (((ca,), (cb,)), ((), ()))

    def one(x, y):
        return lax.dot_general(x, y, dims, preferred_element_type=f32)

    return one(a[0], b[0]) + one(a[1], b[0]) + one(a[0], b[1])


def to_block(rows):
    half = rows.shape[1] // 2
    return jnp.concatenate([rows[:, :half], rows[:, half:]], axis=0)


def from_block(block):
    rows = block.shape[0] // 2
    return jnp.concatenate([block[:rows], block[rows:]], axis=1)


def swap_halves(left, right):
    top = lax.broadcasted_iota(jnp.int32, left.shape, 1) < 4
    return (
        jnp.where(top, left, pltpu.roll(right, 4, 1)),
        jnp.where(top, pltpu.roll(left, 4, 1), right),
    )


def store_blocks(out_ref, at, whole):
    half = whole.shape[1] // 2
    pairs = whole.reshape(whole.shape[0] // 8, 8, whole.shape[1])
    even, odd = swap_halves(pairs[:, :, :half], pairs[:, :, half:])
    both = jnp.stack([even, odd], axis=1)
    out_ref[:, :, at : at + half] = both.reshape(2 * pairs.shape[0], 8, half)


def load_blocks(ref, at, half):
    blocks = ref[:, :, at : at + half]
    pairs = blocks.reshape(blocks.shape[0] // 2, 2, 8, half)
    left, right = swap_halves(pairs[:, 0], pairs[:, 1])
    whole = jnp.concatenate([left, right], axis=2)
    return whole.reshape(whole.shape[0] * 8, 2 * half)


def call(body, out, grid=None, ins=None, outs=None, scratch=(), flops=0, moved=0, name=None):
    kwargs = {}
    if grid is not None:
        kwargs = dict(grid=grid, in_specs=ins, out_specs=outs)
    return pl.pallas_call(
        body,
        out_shape=out,
        scratch_shapes=list(scratch),
        compiler_params=pltpu.CompilerParams(vmem_limit_bytes=40 * MIB),
        cost_estimate=pl.CostEstimate(flops=flops, bytes_accessed=moved, transcendentals=0),
        name=name,
        **kwargs,
    )


def struct(*shape, dtype=f32):
    return jax.ShapeDtypeStruct(shape, dtype)


def full(*shape):
    return pl.BlockSpec(shape, lambda j: (0,) * len(shape))


def spread_first(tok_ref, gain_ref, out_ref):
    x = tok_ref[...]
    n = x * lax.rsqrt(mean(x * x) + eps) * gain_ref[...]
    out_ref[...] = jnp.broadcast_to(to_block(n), out_ref.shape)


def spread(row_ref, out_ref):
    out_ref[...] = jnp.broadcast_to(to_block(row_ref[...]), out_ref.shape)


def spread_last(row_ref, gain_ref, out_ref):
    width = gain_ref.shape[1]
    x = row_ref[:, :width]
    dx = row_ref[:, width:]
    r = lax.rsqrt(mean(x * x) + eps)
    n = x * r * gain_ref[...]
    dn = gain_ref[...] * (dx * r - x * r**3 * mean(x * dx))
    half = width // 2
    out_ref[:, :, :half] = jnp.broadcast_to(to_block(n), (out_ref.shape[0], 8, half))
    out_ref[:, :, half:] = jnp.broadcast_to(to_block(dn), (out_ref.shape[0], 8, half))


def sum_first(blocks_ref, tok_ref, out_ref):
    total = jnp.sum(blocks_ref[...], axis=0)
    half = total.shape[1] // 2
    width = tok_ref.shape[1]
    out_ref[:, :width] = tok_ref[...] + from_block(total[:, :half])
    out_ref[:, width:] = from_block(total[:, half:])


def sum_last(blocks_ref, row_ref, curv_ref, rows_ref, out_ref):
    width = curv_ref.shape[1]
    g = curv_ref[...] * (row_ref[:, width:] + from_block(jnp.sum(blocks_ref[...], axis=0)))
    rows_ref[...] = g
    out_ref[...] = jnp.broadcast_to(to_block(g), out_ref.shape)


def sum_back(blocks_ref, g_ref, row_ref, gain_ref, out_ref):
    width = gain_ref.shape[1]
    u = gain_ref[...] * from_block(jnp.sum(blocks_ref[...], axis=0))
    x = row_ref[:, :width]
    r = lax.rsqrt(mean(x * x) + eps)
    out_ref[...] = g_ref[...] + u * r - x * r**3 * mean(x * u)


def forward(last, blocks_ref, wi_ref, vi_ref, wo_ref, vo_ref, out_ref, nh_ref, nl_ref, ah_ref, al_ref, p_ref, d_ref, *sums):
    j = pl.program_id(0)
    half = nh_ref.shape[1] // 2

    @pl.when(j == 0)
    def _():
        nh_ref[...], nl_ref[...] = parts(load_blocks(blocks_ref, 0, half))
        if last:
            d_ref[0], d_ref[1] = parts(load_blocks(blocks_ref, half, half))

    n = nh_ref[...], nl_ref[...]
    wi = parts(wi_ref[...])
    h = dot3(n, wi)
    dh = dot3(n, parts(vi_ref[...]))
    if last:
        dh = dh + dot3((d_ref[0], d_ref[1]), wi)
    act, slope = gelu_pair(h)
    p_ref[...] = slope
    a = parts(act)
    ah_ref[...], al_ref[...] = a
    da = parts(slope * dh)
    wo = parts(wo_ref[...])
    terms = [dot3(da, wo) + dot3(a, parts(vo_ref[...]))]
    if not last:
        terms.insert(0, dot3(a, wo))
    for sum_ref, term in zip(sums, terms):

        @pl.when(j == 0)
        def _():
            sum_ref[...] = term

        @pl.when(j > 0)
        def _():
            sum_ref[...] += term

    @pl.when(j == pl.num_programs(0) - 1)
    def _():
        for k, sum_ref in enumerate(sums):
            store_blocks(out_ref, k * half, sum_ref[...])


def run_forward(blocks, wi, vi, wo, vo, last):
    chips, _, lanes = blocks.shape
    width, units = wi.shape
    rows = chips * 4
    steps = units // UNITS
    sums = 1 if last else 2
    out_lanes = sums * width // 2
    inward = pl.BlockSpec((width, UNITS), lambda j: (0, j))
    outward = pl.BlockSpec((UNITS, width), lambda j: (j, 0))
    held = pl.BlockSpec((rows, UNITS), lambda j: (0, j))
    return call(
        functools.partial(forward, last),
        (
            struct(chips, 8, out_lanes),
            struct(rows, width, dtype=bf16),
            struct(rows, width, dtype=bf16),
            struct(rows, units, dtype=bf16),
            struct(rows, units, dtype=bf16),
            struct(rows, units),
        ),
        grid=(steps,),
        ins=[full(chips, 8, lanes), inward, inward, outward, outward],
        outs=(full(chips, 8, out_lanes), full(rows, width), full(rows, width), held, held, held),
        scratch=[pltpu.VMEM((2, rows, width) if last else (2, 8, 128), bf16)]
        + [pltpu.VMEM((rows, width), f32)] * sums,
        flops=2 * rows * width * units * 5 * 3,
        moved=4 * width * units * 4,
        name="forward_last" if last else "forward_first",
    )(blocks, wi, vi, wo, vo)


def backward(with_input, blocks_ref, p_ref, wo_ref, *refs):
    if with_input:
        wi_ref, gh_ref, gl_ref, eh_ref, el_ref, out_ref, u_ref = refs
    else:
        gh_ref, gl_ref, eh_ref, el_ref = refs
    j = pl.program_id(0)
    half = gh_ref.shape[1] // 2

    @pl.when(j == 0)
    def _():
        gh_ref[...], gl_ref[...] = parts(load_blocks(blocks_ref, 0, half))

    g = gh_ref[...], gl_ref[...]
    e = parts(p_ref[...] * dot3(g, parts(wo_ref[...]), 1, 1))
    eh_ref[...], el_ref[...] = e
    if with_input:
        u = dot3(e, parts(wi_ref[...]), 1, 1)

        @pl.when(j == 0)
        def _():
            u_ref[...] = u

        @pl.when(j > 0)
        def _():
            u_ref[...] += u

        @pl.when(j == pl.num_programs(0) - 1)
        def _():
            store_blocks(out_ref, 0, u_ref[...])


def run_backward(blocks, p, wo, wi=None):
    chips, _, lanes = blocks.shape
    units, width = wo.shape
    rows = chips * 4
    inward = pl.BlockSpec((width, UNITS), lambda j: (0, j))
    outward = pl.BlockSpec((UNITS, width), lambda j: (j, 0))
    held = pl.BlockSpec((rows, UNITS), lambda j: (0, j))
    more = wi is not None
    whole = full(rows, width)
    return call(
        functools.partial(backward, more),
        (
            struct(rows, width, dtype=bf16),
            struct(rows, width, dtype=bf16),
            struct(rows, units, dtype=bf16),
            struct(rows, units, dtype=bf16),
        )
        + ((struct(chips, 8, lanes),) if more else ()),
        grid=(units // UNITS,),
        ins=[full(chips, 8, lanes), held, outward] + ([inward] if more else []),
        outs=(whole, whole, held, held) + ((full(chips, 8, lanes),) if more else ()),
        scratch=[pltpu.VMEM((rows, width), f32)] if more else [],
        flops=2 * rows * width * units * 3 * (2 if more else 1),
        moved=4 * width * units * (2 if more else 1),
        name="backward_last" if more else "backward_first",
    )(*((blocks, p, wo) + ((wi,) if more else ())))


def products(nh_ref, nl_ref, ah_ref, al_ref, eh_ref, el_ref, gh_ref, gl_ref, in_ref, out_ref):
    out_ref[...] = dot3((ah_ref[...], al_ref[...]), (gh_ref[...], gl_ref[...]), 0, 0)
    in_ref[...] = dot3((nh_ref[...], nl_ref[...]), (eh_ref[...], el_ref[...]), 0, 0)


def run_products(n, a, e, g):
    rows, width = n[0].shape
    units = a[0].shape[1]
    held = pl.BlockSpec((rows, UNITS), lambda j: (0, j))
    whole = full(rows, width)
    return call(
        products,
        (struct(width, units), struct(units, width)),
        grid=(units // UNITS,),
        ins=[whole, whole, held, held, held, held, whole, whole],
        outs=(
            pl.BlockSpec((width, UNITS), lambda j: (0, j)),
            pl.BlockSpec((UNITS, width), lambda j: (j, 0)),
        ),
        flops=2 * rows * width * units * 6,
        moved=8 * width * units,
        name="products",
    )(*n, *a, *e, *g)


def exchanged(blocks):
    return lax.all_to_all(blocks, "mp", 0, 0, tiled=True)


def on_device(tokens, curvature, gains, w_in, w_out, v_in, v_out):
    first = lax.axis_index("segment") == 0
    gain, wi, wo, vi, vo = gains, w_in[0], w_out[0], v_in[0], v_out[0]
    width = tokens.shape[2]
    x0 = tokens.reshape(-1, width)
    curv = curvature.reshape(-1, width)
    rows = x0.shape[0]
    chips = lax.axis_size("mp")
    total = rows * chips
    units = wi.shape[1]
    single = struct(chips, 8, width // 2)
    double = struct(chips, 8, width)

    def blank(*shape, dtype=f32):
        return jnp.zeros(shape, dtype)

    def blanks(count, columns):
        return tuple(blank(total, columns, dtype=bf16) for _ in range(count))

    def forward_first():
        blocks = exchanged(call(spread_first, single, name="spread_first")(x0, gain))
        out, nh, nl, ah, al, p = run_forward(blocks, wi, vi, wo, vo, False)
        rows_out = call(sum_first, struct(rows, 2 * width), name="sum_first")(exchanged(out), x0)
        return rows_out, nh, nl, ah, al, p

    def no_forward():
        return (blank(rows, 2 * width), *blanks(2, width), *blanks(2, units), blank(total, units))

    both, *held = lax.cond(first, forward_first, no_forward)
    p0 = held.pop()
    both = lax.ppermute(both, "segment", [(0, 1)])

    def layer_last(both, *held):
        blocks = exchanged(call(spread_last, double, name="spread_last")(both, gain))
        out, nh, nl, ah, al, p = run_forward(blocks, wi, vi, wo, vo, True)
        g, blocks = call(sum_last, (struct(rows, width), single), name="sum_last")(
            exchanged(out), both, curv
        )
        gh, gl, eh, el, out = run_backward(exchanged(blocks), p, wo, wi)
        back = call(sum_back, struct(rows, width), name="sum_back")(exchanged(out), g, both, gain)
        return back, nh, nl, ah, al, eh, el, gh, gl

    def keep(both, *held):
        return (blank(rows, width), *held, *blanks(2, units), *blanks(2, width))

    back, nh, nl, ah, al, *rest = lax.cond(first, keep, layer_last, both, *held)
    back = lax.ppermute(back, "segment", [(1, 0)])

    def backward_first(back, *rest):
        blocks = exchanged(call(spread, single, name="spread")(back))
        gh, gl, eh, el = run_backward(blocks, p0, wo)
        return eh, el, gh, gl

    def pass_on(back, *rest):
        return rest

    eh, el, gh, gl = lax.cond(first, backward_first, pass_on, back, *rest)

    product_in, product_out = run_products((nh, nl), (ah, al), (eh, el), (gh, gl))
    return product_in[None], product_out[None]


def solution(mesh):
    rows = P(None, "mp", None)
    layer_in = P("segment", None, "mp")
    layer_out = P("segment", "mp", None)
    return jax.shard_map(
        on_device,
        mesh=mesh,
        in_specs=(rows, rows, P("segment", None), layer_in, layer_out, layer_in, layer_out),
        out_specs=(layer_in, layer_out),
        check_vma=False,
    )
```

```python
import functools

import jax
import jax.numpy as jnp
from jax import lax
from jax.experimental import pallas as pl
from jax.experimental.pallas import tpu as pltpu
from jax.sharding import PartitionSpec as P

eps = 1e-06
coeff = 0.7978845608028654
f32 = jnp.float32
bf16 = jnp.bfloat16
UNITS = 256
MIB = 1 << 20
LANES = 128
GROUP = 4
PIECES = 2
COVER_FLOPS = 1 << 34


def gelu_pair(h):
    inner = coeff * (h + 0.044715 * h * h * h)
    tval = jnp.tanh(inner)
    act = 0.5 * h * (1.0 + tval)
    slope = 0.5 * (1.0 + tval) + 0.5 * h * (1.0 - tval * tval) * coeff * (
        1.0 + 3.0 * 0.044715 * h * h
    )
    return act, slope


def mean(v):
    return jnp.mean(v, axis=-1, keepdims=True)


def parts(v):
    high = v.astype(bf16)
    return high, (v - high.astype(f32)).astype(bf16)


def dot3(a, b, ca=1, cb=0):
    dims = (((ca,), (cb,)), ((), ()))

    def one(x, y):
        return lax.dot_general(x, y, dims, preferred_element_type=f32)

    return one(a[0], b[0]) + one(a[1], b[0]) + one(a[0], b[1])


def to_block(rows):
    half = rows.shape[1] // 2
    return jnp.concatenate([rows[:, :half], rows[:, half:]], axis=0)


def from_block(block):
    rows = block.shape[0] // 2
    return jnp.concatenate([block[:rows], block[rows:]], axis=1)


def swap_halves(left, right):
    top = lax.broadcasted_iota(jnp.int32, left.shape, 1) < 4
    return (
        jnp.where(top, left, pltpu.roll(right, 4, 1)),
        jnp.where(top, pltpu.roll(left, 4, 1), right),
    )


def load_blocks(ref, at, half):
    blocks = ref[:, :, at : at + half]
    pairs = blocks.reshape(blocks.shape[0] // 2, 2, 8, half)
    left, right = swap_halves(pairs[:, 0], pairs[:, 1])
    whole = jnp.concatenate([left, right], axis=2)
    return whole.reshape(whole.shape[0] * 8, 2 * half)


def call(body, out, grid=None, ins=None, outs=None, scratch=(), flops=0, moved=0, limit=12, name=None):
    kwargs = {}
    if grid is not None:
        kwargs["grid"] = grid
    if ins is not None:
        kwargs.update(in_specs=ins, out_specs=outs)
    return pl.pallas_call(
        body,
        out_shape=out,
        scratch_shapes=list(scratch),
        compiler_params=pltpu.CompilerParams(vmem_limit_bytes=limit * MIB),
        cost_estimate=pl.CostEstimate(flops=flops, bytes_accessed=moved, transcendentals=0),
        name=name,
        **kwargs,
    )


here = pl.BlockSpec(memory_space=pltpu.VMEM)
there = pl.BlockSpec(memory_space=pl.ANY)


def struct(*shape, dtype=f32):
    return jax.ShapeDtypeStruct(shape, dtype)


def flat(ref):
    return jnp.concatenate([ref[0], ref[1]], axis=0)


def spread_first(tok_ref, gain_ref, out_ref):
    x = flat(tok_ref)
    n = x * lax.rsqrt(mean(x * x) + eps) * gain_ref[...]
    out_ref[...] = jnp.broadcast_to(to_block(n), out_ref.shape)


def spread(row_ref, out_ref):
    out_ref[...] = jnp.broadcast_to(to_block(row_ref[...]), out_ref.shape)


def spread_last(row_ref, gain_ref, out_ref):
    width = gain_ref.shape[1]
    x = row_ref[:, :width]
    dx = row_ref[:, width:]
    r = lax.rsqrt(mean(x * x) + eps)
    n = x * r * gain_ref[...]
    dn = gain_ref[...] * (dx * r - x * r**3 * mean(x * dx))
    half = width // 2
    out_ref[:, :, :half] = jnp.broadcast_to(to_block(n), (out_ref.shape[0], 8, half))
    out_ref[:, :, half:] = jnp.broadcast_to(to_block(dn), (out_ref.shape[0], 8, half))


def sum_first(blocks_ref, tok_ref, out_ref):
    total = jnp.sum(blocks_ref[...], axis=0)
    half = total.shape[1] // 2
    width = tok_ref.shape[2]
    out_ref[:, :width] = flat(tok_ref) + from_block(total[:, :half])
    out_ref[:, width:] = from_block(total[:, half:])


def sum_last(blocks_ref, row_ref, curv_ref, rows_ref, out_ref):
    width = curv_ref.shape[2]
    g = flat(curv_ref) * (row_ref[:, width:] + from_block(jnp.sum(blocks_ref[...], axis=0)))
    rows_ref[...] = g
    out_ref[...] = jnp.broadcast_to(to_block(g), out_ref.shape)


def sum_back(blocks_ref, g_ref, row_ref, gain_ref, out_ref):
    width = gain_ref.shape[1]
    u = gain_ref[...] * from_block(jnp.sum(blocks_ref[...], axis=0))
    x = row_ref[:, :width]
    r = lax.rsqrt(mean(x * x) + eps)
    out_ref[...] = g_ref[...] + u * r - x * r**3 * mean(x * u)


def split(*refs):
    half = len(refs) // 2
    for in_ref, out_ref in zip(refs[:half], refs[half:]):
        keep_parts(out_ref, in_ref[...])


def run_split(*weights):
    rows, columns = weights[0].shape
    step = 256
    count = len(weights)
    return call(
        split,
        (struct(*tiled(rows, columns), dtype=bf16),) * count,
        grid=(rows // step,),
        ins=[pl.BlockSpec((step, columns), lambda j: (j, 0))] * count,
        outs=(pl.BlockSpec(tiled(step, columns), lambda j: (0, 0, j, 0)),) * count,
        flops=COVER_FLOPS,
        moved=8 * rows * columns * count,
        limit=26,
        name="split",
    )(*weights)


def turn(n_ref, a_ref, nt_ref, at_ref):
    for ref, turned in ((n_ref, nt_ref), (a_ref, at_ref)):
        for b in range(ref.shape[1]):
            for k in range(2):
                t = ref[k, b].T
                for c in range(turned.shape[1]):
                    turned[k, c, b * LANES : (b + 1) * LANES, :] = t[:, c * LANES : (c + 1) * LANES]


def run_turn(n, a):
    return call(
        turn,
        tuple(struct(*tiled(v.shape[1] * LANES, v.shape[2]), dtype=bf16) for v in (n, a)),
        flops=COVER_FLOPS,
        moved=4 * (n.size + a.size),
        limit=12,
        name="turn",
    )(n, a)


def tiled(rows, columns):
    return 2, columns // LANES, rows, LANES


def groups(ref, columns):
    first, last = (0, ref.shape[1] * LANES) if columns is None else (columns.start, columns.stop)
    return slice(first // LANES, last // LANES)


def cut(ref, rows=slice(None), columns=None):
    some = groups(ref, columns)
    return tuple(
        jnp.concatenate([ref[k, b, rows, :] for b in range(some.start, some.stop)], axis=1) for k in range(2)
    )


def keep_parts(ref, value, rows=slice(None), columns=None):
    some = groups(ref, columns)
    for k, part in enumerate(parts(value)):
        for at, b in enumerate(range(some.start, some.stop)):
            ref[k, b, rows, :] = part[:, at * LANES : (at + 1) * LANES]


def blocks_of(size):
    return [slice(at, at + UNITS) for at in range(0, size, UNITS)]


def output_columns(width):
    half = width // 2
    return [(at, slice(at, at + UNITS), slice(half + at, half + at + UNITS)) for at in range(0, half, UNITS)]


def store_pair(out_ref, at, left, right):
    rows, lanes = left.shape
    even, odd = swap_halves(left.reshape(rows // 8, 8, lanes), right.reshape(rows // 8, 8, lanes))
    out_ref[:, :, at : at + lanes] = jnp.stack([even, odd], axis=1).reshape(rows // 4, 8, lanes)


class Copies:
    def __init__(self, sems, sets=()):
        self.sems = sems
        self.count = 0
        self.sets = list(sets)
        self.begun = []

    def start(self, source, target):
        copy = pltpu.make_async_copy(source, target, self.sems.at[self.count])
        self.count += 1
        copy.start()
        return copy

    def begin(self, upto):
        for pairs in self.sets[len(self.begun) : upto]:
            self.begun.append([self.start(*pair) for pair in pairs])

    def wait(self, first, last):
        self.begin(last)
        for begun in self.begun[first:last]:
            wait(*begun)


def wait(*copies):
    for copy in copies:
        copy.wait()


def forward(last, blocks_ref, wi_hbm, vi_hbm, wo_hbm, vo_hbm, out_ref, n_hbm, a_hbm, p_hbm, *scratch):
    wi, vi, wo, vo, n, a, p, da, d, sems = scratch
    width, units = wi.shape[2], p.shape[1]
    half = width // 2

    def pair(first, second, cols):
        return [(source.at[:, groups(source, cols)], target.at[:, groups(target, cols)]) for source, target in (first, second)]

    inward = [pair((wi_hbm, wi), (vi_hbm, vi), c) for c in blocks_of(units)]
    outward = [
        pair((wo_hbm, wo), (vo_hbm, vo), c) for _, *both in output_columns(width) for c in both
    ]
    copies = Copies(sems, inward + outward)
    copies.begin(GROUP)
    keep_parts(n, load_blocks(blocks_ref, 0, half))
    copies.begin(2 * GROUP)
    if last:
        keep_parts(d, load_blocks(blocks_ref, half, half))
    for k, cols in enumerate(blocks_of(units)):
        if k % GROUP == 0:
            copies.wait(k, k + GROUP)
            copies.begin(k + 3 * GROUP)
        h = dot3(cut(n), cut(wi, columns=cols))
        dh = dot3(cut(n), cut(vi, columns=cols))
        if last:
            dh = dh + dot3(cut(d), cut(wi, columns=cols))
        act, slope = gelu_pair(h)
        p[:, cols] = slope
        keep_parts(a, act, columns=cols)
        keep_parts(da, slope * dh, columns=cols)
    results = [copies.start(n, n_hbm), copies.start(a, a_hbm), copies.start(p, p_hbm)]
    copies.wait(len(inward), len(copies.sets))
    for at, left, right in output_columns(width):
        if not last:
            store_pair(out_ref, at, *(dot3(cut(a), cut(wo, columns=c)) for c in (left, right)))
        terms = [
            dot3(cut(da), cut(wo, columns=c)) + dot3(cut(a), cut(vo, columns=c)) for c in (left, right)
        ]
        store_pair(out_ref, at + (0 if last else half), *terms)
    wait(*results)


def run_forward(blocks, weights, last):
    chips, _, lanes = blocks.shape
    width, units = weights[0].shape[2], weights[2].shape[2]
    rows = chips * 4
    out_lanes = (1 if last else 2) * width // 2
    inward = pltpu.VMEM(tiled(width, units), bf16)
    outward = pltpu.VMEM(tiled(units, width), bf16)
    small = pltpu.VMEM(tiled(rows, width), bf16)
    wide = pltpu.VMEM(tiled(rows, units), bf16)
    copies = 2 * (units // UNITS) + 2 * (width // UNITS) + 3
    return call(
        functools.partial(forward, last),
        (
            struct(chips, 8, out_lanes),
            struct(*tiled(rows, width), dtype=bf16),
            struct(*tiled(rows, units), dtype=bf16),
            struct(rows, units),
        ),
        ins=[here] + [there] * 4,
        outs=(here,) + (there,) * 3,
        scratch=[inward, inward, outward, outward, small, wide, pltpu.VMEM((rows, units), f32), wide]
        + [small if last else pltpu.VMEM((8, 128), bf16), pltpu.SemaphoreType.DMA((copies,))],
        flops=2 * rows * width * units * 5 * 3,
        moved=4 * width * units * 4,
        limit=40,
        name="forward_last" if last else "forward_first",
    )(blocks, *weights)


def backward(blocks_ref, p_hbm, wo_hbm, wi_hbm, out_ref, p, wo, wi, g, e, sems):
    units, width = wo.shape[2], wi.shape[2]
    first = [
        [(wo_hbm.at[:, :, c, :], wo.at[:, :, c, :]), (p_hbm.at[:, c], p.at[:, c])] for c in blocks_of(units)
    ]
    second = [
        [(wi_hbm.at[:, :, c, :], wi.at[:, :, c, :]) for c in (left, right)]
        for _, left, right in output_columns(width)
    ]
    copies = Copies(sems, first + second)
    copies.begin(len(first))
    keep_parts(g, load_blocks(blocks_ref, 0, width // 2))
    copies.wait(0, len(first))
    copies.begin(len(copies.sets))
    for c in blocks_of(units):
        keep_parts(e, p[:, c] * dot3(cut(g), cut(wo, rows=c), 1, 1), columns=c)
    copies.wait(len(first), len(copies.sets))
    for at, left, right in output_columns(width):
        store_pair(out_ref, at, *(dot3(cut(e), cut(wi, rows=c), 1, 1) for c in (left, right)))


def run_backward(blocks, p, wo, wi):
    chips, _, lanes = blocks.shape
    units, width = wo.shape[2], wi.shape[2]
    rows = chips * 4
    return call(
        backward,
        struct(chips, 8, lanes),
        ins=[here] + [there] * 3,
        outs=here,
        scratch=[
            pltpu.VMEM((rows, units), f32),
            pltpu.VMEM(tiled(units, width), bf16),
            pltpu.VMEM(tiled(width, units), bf16),
            pltpu.VMEM(tiled(rows, width), bf16),
            pltpu.VMEM(tiled(rows, units), bf16),
            pltpu.SemaphoreType.DMA((2 * (units // UNITS) + width // UNITS,)),
        ],
        flops=2 * rows * width * units * 6,
        moved=8 * width * units,
        limit=24,
        name="backward_last",
    )(blocks, p, wo, wi)


def finish(blocks_ref, p_hbm, wo_hbm, at_hbm, nt_hbm, in_hbm, out_hbm, *scratch):
    p, wo, at, nt, g, e, of_in, of_out, sems = scratch
    units, width = p.shape[1], nt.shape[2]
    sets = [[(at_hbm, at)], [(wo_hbm, wo), (p_hbm, p)], [(nt_hbm, nt)]]
    copies = Copies(sems, sets)
    copies.begin(2)
    keep_parts(g, load_blocks(blocks_ref, 0, width // 2))
    results = []

    def put(source, target, rows):
        step = UNITS // PIECES
        for first in range(rows.start, rows.stop, step):
            some = slice(first, first + step)
            results.append(copies.start(source.at[some, :], target.at[some, :]))

    copies.wait(0, 1)
    copies.begin(3)
    for c in blocks_of(units):
        of_out[c, :] = dot3(cut(at, rows=c), cut(g))
        put(of_out, out_hbm, c)
    copies.wait(1, 3)
    for c in blocks_of(units):
        keep_parts(e, p[:, c] * dot3(cut(g), cut(wo, rows=c), 1, 1), columns=c)
    for c in blocks_of(width):
        of_in[c, :] = dot3(cut(nt, rows=c), cut(e))
        put(of_in, in_hbm, c)
    wait(*results)


def run_finish(blocks, p, wo, at, nt):
    units, width = at.shape[2], nt.shape[2]
    rows = at.shape[1] * LANES
    return call(
        finish,
        (struct(width, units), struct(units, width)),
        ins=[here] + [there] * 4,
        outs=(there, there),
        scratch=[
            pltpu.VMEM((rows, units), f32),
            pltpu.VMEM(tiled(units, width), bf16),
            pltpu.VMEM(tiled(units, rows), bf16),
            pltpu.VMEM(tiled(width, rows), bf16),
            pltpu.VMEM(tiled(rows, width), bf16),
            pltpu.VMEM(tiled(rows, units), bf16),
            pltpu.VMEM((width, units), f32),
            pltpu.VMEM((units, width), f32),
            pltpu.SemaphoreType.DMA((4 + PIECES * (units + width) // UNITS,)),
        ],
        flops=2 * rows * width * units * 9,
        moved=12 * width * units,
        limit=36,
        name="finish",
    )(blocks, p, wo, at, nt)


def exchanged(blocks):
    return lax.all_to_all(blocks, "mp", 0, 0, tiled=True)


def on_device(tokens, curvature, gains, w_in, w_out, v_in, v_out):
    first = lax.axis_index("segment") == 0
    gain = gains
    weights = w_in[0], v_in[0], w_out[0], v_out[0]
    width = tokens.shape[2]
    rows = tokens.shape[0] * tokens.shape[1]
    chips = lax.axis_size("mp")
    total = rows * chips
    units = w_in.shape[2]
    single = struct(chips, 8, width // 2)
    double = struct(chips, 8, width)

    def blank(*shape, dtype=f32):
        return jnp.zeros(shape, dtype)

    def forward_first():
        blocks = exchanged(call(spread_first, single, name="spread_first")(tokens, gain))
        split_weights = run_split(*weights)
        out, n, a, p = run_forward(blocks, split_weights, False)
        both = call(sum_first, struct(rows, 2 * width), name="sum_first")(exchanged(out), tokens)
        return both, n, a, p, split_weights

    def no_forward():
        return (
            blank(rows, 2 * width),
            blank(*tiled(total, width), dtype=bf16),
            blank(*tiled(total, units), dtype=bf16),
            blank(total, units),
            run_split(*weights),
        )

    both, n0, a0, p0, split_weights = lax.cond(first, forward_first, no_forward)
    both = lax.ppermute(both, "segment", [(0, 1)])

    def layer_last(both, n0, a0, p0, split_weights):
        blocks = exchanged(call(spread_last, double, name="spread_last")(both, gain))
        out, n, a, p = run_forward(blocks, split_weights, True)
        g, blocks = call(sum_last, (struct(rows, width), single), name="sum_last")(
            exchanged(out), both, curvature
        )
        blocks = exchanged(blocks)
        out = run_backward(blocks, p, split_weights[2], split_weights[0])
        back = call(sum_back, struct(rows, width), name="sum_back")(exchanged(out), g, both, gain)
        return back, blocks, p, *run_turn(n, a)

    def keep(both, n0, a0, p0, split_weights):
        return blank(rows, width), blank(*single.shape), p0, *run_turn(n0, a0)

    back, blocks, p, nt, at = lax.cond(first, keep, layer_last, both, n0, a0, p0, split_weights)
    back = lax.ppermute(back, "segment", [(1, 0)])

    def cotangent_first(back, blocks):
        return exchanged(call(spread, single, name="spread")(back))

    def pass_on(back, blocks):
        return blocks

    blocks = lax.cond(first, cotangent_first, pass_on, back, blocks)

    product_in, product_out = run_finish(blocks, p, split_weights[2], at, nt)
    return product_in[None], product_out[None]


def solution(mesh):
    rows = P(None, "mp", None)
    layer_in = P("segment", None, "mp")
    layer_out = P("segment", "mp", None)
    return jax.shard_map(
        on_device,
        mesh=mesh,
        in_specs=(rows, rows, P("segment", None), layer_in, layer_out, layer_in, layer_out),
        out_specs=(layer_in, layer_out),
        check_vma=False,
    )
```

```python
import functools

import jax
import jax.numpy as jnp
from jax import lax
from jax.experimental import pallas as pl
from jax.experimental.pallas import tpu as pltpu
from jax.sharding import PartitionSpec as P

eps = 1e-06
coeff = 0.7978845608028654
f32 = jnp.float32
bf16 = jnp.bfloat16
UNITS = 256
MIB = 1 << 20
LANES = 128
GROUP = 4
PIECES = 2
COVER_FLOPS = 1 << 34


def gelu_pair(h):
    inner = coeff * (h + 0.044715 * h * h * h)
    tval = jnp.tanh(inner)
    act = 0.5 * h * (1.0 + tval)
    slope = 0.5 * (1.0 + tval) + 0.5 * h * (1.0 - tval * tval) * coeff * (
        1.0 + 3.0 * 0.044715 * h * h
    )
    return act, slope


def mean(v):
    return jnp.mean(v, axis=-1, keepdims=True)


def parts(v):
    high = v.astype(bf16)
    return high, (v - high.astype(f32)).astype(bf16)


def dot3(a, b, ca=1, cb=0):
    dims = (((ca,), (cb,)), ((), ()))

    def one(x, y):
        return lax.dot_general(x, y, dims, preferred_element_type=f32)

    return one(a[0], b[0]) + one(a[1], b[0]) + one(a[0], b[1])


def to_block(rows):
    half = rows.shape[1] // 2
    return jnp.concatenate([rows[:, :half], rows[:, half:]], axis=0)


def from_block(block):
    rows = block.shape[0] // 2
    return jnp.concatenate([block[:rows], block[rows:]], axis=1)


def swap_halves(left, right):
    top = lax.broadcasted_iota(jnp.int32, left.shape, 1) < 4
    return (
        jnp.where(top, left, pltpu.roll(right, 4, 1)),
        jnp.where(top, pltpu.roll(left, 4, 1), right),
    )


def load_blocks(ref, at, half):
    blocks = ref[:, :, at : at + half]
    pairs = blocks.reshape(blocks.shape[0] // 2, 2, 8, half)
    left, right = swap_halves(pairs[:, 0], pairs[:, 1])
    whole = jnp.concatenate([left, right], axis=2)
    return whole.reshape(whole.shape[0] * 8, 2 * half)


def call(body, out, grid=None, ins=None, outs=None, scratch=(), flops=0, moved=0, limit=12, name=None):
    kwargs = {}
    if grid is not None:
        kwargs["grid"] = grid
    if ins is not None:
        kwargs.update(in_specs=ins, out_specs=outs)
    return pl.pallas_call(
        body,
        out_shape=out,
        scratch_shapes=list(scratch),
        compiler_params=pltpu.CompilerParams(vmem_limit_bytes=limit * MIB),
        cost_estimate=pl.CostEstimate(flops=flops, bytes_accessed=moved, transcendentals=0),
        name=name,
        **kwargs,
    )


here = pl.BlockSpec(memory_space=pltpu.VMEM)
there = pl.BlockSpec(memory_space=pl.ANY)


def struct(*shape, dtype=f32):
    return jax.ShapeDtypeStruct(shape, dtype)


def flat(ref):
    return jnp.concatenate([ref[0], ref[1]], axis=0)


def spread_first(tok_ref, gain_ref, out_ref):
    x = flat(tok_ref)
    n = x * lax.rsqrt(mean(x * x) + eps) * gain_ref[...]
    out_ref[...] = jnp.broadcast_to(to_block(n), out_ref.shape)


def spread(row_ref, out_ref):
    out_ref[...] = jnp.broadcast_to(to_block(row_ref[...]), out_ref.shape)


def spread_last(row_ref, gain_ref, out_ref):
    width = gain_ref.shape[1]
    x = row_ref[:, :width]
    dx = row_ref[:, width:]
    r = lax.rsqrt(mean(x * x) + eps)
    n = x * r * gain_ref[...]
    dn = gain_ref[...] * (dx * r - x * r**3 * mean(x * dx))
    half = width // 2
    out_ref[:, :, :half] = jnp.broadcast_to(to_block(n), (out_ref.shape[0], 8, half))
    out_ref[:, :, half:] = jnp.broadcast_to(to_block(dn), (out_ref.shape[0], 8, half))


def sum_first(blocks_ref, tok_ref, out_ref):
    total = jnp.sum(blocks_ref[...], axis=0)
    half = total.shape[1] // 2
    width = tok_ref.shape[2]
    out_ref[:, :width] = flat(tok_ref) + from_block(total[:, :half])
    out_ref[:, width:] = from_block(total[:, half:])


def sum_last(blocks_ref, row_ref, curv_ref, rows_ref, out_ref):
    width = curv_ref.shape[2]
    g = flat(curv_ref) * (row_ref[:, width:] + from_block(jnp.sum(blocks_ref[...], axis=0)))
    rows_ref[...] = g
    out_ref[...] = jnp.broadcast_to(to_block(g), out_ref.shape)


def sum_back(blocks_ref, g_ref, row_ref, gain_ref, out_ref):
    width = gain_ref.shape[1]
    u = gain_ref[...] * from_block(jnp.sum(blocks_ref[...], axis=0))
    x = row_ref[:, :width]
    r = lax.rsqrt(mean(x * x) + eps)
    out_ref[...] = g_ref[...] + u * r - x * r**3 * mean(x * u)


def split(*refs):
    half = len(refs) // 2
    for in_ref, out_ref in zip(refs[:half], refs[half:]):
        keep_parts(out_ref, in_ref[...])


def run_split(*weights):
    rows, columns = weights[0].shape
    step = 256
    count = len(weights)
    return call(
        split,
        (struct(*tiled(rows, columns), dtype=bf16),) * count,
        grid=(rows // step,),
        ins=[pl.BlockSpec((step, columns), lambda j: (j, 0))] * count,
        outs=(pl.BlockSpec(tiled(step, columns), lambda j: (0, 0, j, 0)),) * count,
        flops=COVER_FLOPS,
        moved=8 * rows * columns * count,
        limit=26,
        name="split",
    )(*weights)


def turn(n_ref, a_ref, nt_ref, at_ref):
    for ref, turned in ((n_ref, nt_ref), (a_ref, at_ref)):
        for b in range(ref.shape[1]):
            for k in range(2):
                t = ref[k, b].T
                for c in range(turned.shape[1]):
                    turned[k, c, b * LANES : (b + 1) * LANES, :] = t[:, c * LANES : (c + 1) * LANES]


def run_turn(n, a):
    return call(
        turn,
        tuple(struct(*tiled(v.shape[1] * LANES, v.shape[2]), dtype=bf16) for v in (n, a)),
        flops=COVER_FLOPS,
        moved=4 * (n.size + a.size),
        limit=12,
        name="turn",
    )(n, a)


def tiled(rows, columns):
    return 2, columns // LANES, rows, LANES


def groups(ref, columns):
    first, last = (0, ref.shape[1] * LANES) if columns is None else (columns.start, columns.stop)
    return slice(first // LANES, last // LANES)


def cut(ref, rows=slice(None), columns=None):
    some = groups(ref, columns)
    return tuple(
        jnp.concatenate([ref[k, b, rows, :] for b in range(some.start, some.stop)], axis=1) for k in range(2)
    )


def keep_parts(ref, value, rows=slice(None), columns=None):
    some = groups(ref, columns)
    for k, part in enumerate(parts(value)):
        for at, b in enumerate(range(some.start, some.stop)):
            ref[k, b, rows, :] = part[:, at * LANES : (at + 1) * LANES]


def blocks_of(size):
    return [slice(at, at + UNITS) for at in range(0, size, UNITS)]


def output_columns(width):
    half = width // 2
    return [(at, slice(at, at + UNITS), slice(half + at, half + at + UNITS)) for at in range(0, half, UNITS)]


def store_pair(out_ref, at, left, right):
    rows, lanes = left.shape
    even, odd = swap_halves(left.reshape(rows // 8, 8, lanes), right.reshape(rows // 8, 8, lanes))
    out_ref[:, :, at : at + lanes] = jnp.stack([even, odd], axis=1).reshape(rows // 4, 8, lanes)


class Copies:
    def __init__(self, sems, sets=()):
        self.sems = sems
        self.count = 0
        self.sets = list(sets)
        self.begun = []

    def start(self, source, target):
        copy = pltpu.make_async_copy(source, target, self.sems.at[self.count])
        self.count += 1
        copy.start()
        return copy

    def begin(self, upto):
        for pairs in self.sets[len(self.begun) : upto]:
            self.begun.append([self.start(*pair) for pair in pairs])

    def wait(self, first, last):
        self.begin(last)
        for begun in self.begun[first:last]:
            wait(*begun)


def wait(*copies):
    for copy in copies:
        copy.wait()


def forward(last, blocks_ref, wi_hbm, vi_hbm, wo_hbm, vo_hbm, out_ref, n_hbm, a_hbm, p_hbm, *scratch):
    wi, vi, wo, vo, n, a, p, da, d, sems = scratch
    units, width = wo.shape
    half = width // 2

    def pair(first, second, cols):
        if len(first[0].shape) == 2:
            return [(source.at[:, cols], target.at[:, cols]) for source, target in (first, second)]
        return [
            (source.at[:, groups(source, cols)], target.at[:, groups(target, cols)])
            for source, target in (first, second)
        ]

    inward = [pair((wi_hbm, wi), (vi_hbm, vi), c) for c in blocks_of(units)]
    outward = [
        pair((wo_hbm, wo), (vo_hbm, vo), c) for _, *both in output_columns(width) for c in both
    ]
    copies = Copies(sems, inward + outward)
    copies.begin(GROUP)
    keep_parts(n, load_blocks(blocks_ref, 0, half))
    if last:
        keep_parts(d, load_blocks(blocks_ref, half, half))
    for k, cols in enumerate(blocks_of(units)):
        if k % GROUP == 0:
            copies.wait(k, k + GROUP)
            copies.begin(k + 3 * GROUP)
        h = dot3(cut(n), cut(wi, columns=cols))
        dh = dot3(cut(n), cut(vi, columns=cols))
        if last:
            dh = dh + dot3(cut(d), cut(wi, columns=cols))
        act, slope = gelu_pair(h)
        p[:, cols] = slope
        keep_parts(a, act, columns=cols)
        keep_parts(da, slope * dh, columns=cols)
    results = [copies.start(n, n_hbm), copies.start(a, a_hbm), copies.start(p, p_hbm)]
    copies.wait(len(inward), len(copies.sets))
    for at, left, right in output_columns(width):
        wo_here = [parts(wo[:, c]) for c in (left, right)]
        if not last:
            store_pair(out_ref, at, *(dot3(cut(a), w) for w in wo_here))
        terms = [
            dot3(cut(da), w) + dot3(cut(a), parts(vo[:, c])) for w, c in zip(wo_here, (left, right))
        ]
        store_pair(out_ref, at + (0 if last else half), *terms)
    wait(*results)


def run_forward(blocks, weights, last):
    chips, _, lanes = blocks.shape
    units, width = weights[2].shape
    rows = chips * 4
    out_lanes = (1 if last else 2) * width // 2
    inward = pltpu.VMEM(tiled(width, units), bf16)
    outward = pltpu.VMEM((units, width), f32)
    small = pltpu.VMEM(tiled(rows, width), bf16)
    wide = pltpu.VMEM(tiled(rows, units), bf16)
    copies = 2 * (units // UNITS) + 2 * (width // UNITS) + 3
    return call(
        functools.partial(forward, last),
        (
            struct(chips, 8, out_lanes),
            struct(*tiled(rows, width), dtype=bf16),
            struct(*tiled(rows, units), dtype=bf16),
            struct(rows, units),
        ),
        ins=[here] + [there] * 4,
        outs=(here,) + (there,) * 3,
        scratch=[inward, inward, outward, outward, small, wide, pltpu.VMEM((rows, units), f32), wide]
        + [small if last else pltpu.VMEM((8, 128), bf16), pltpu.SemaphoreType.DMA((copies,))],
        flops=2 * rows * width * units * 5 * 3,
        moved=4 * width * units * 4,
        limit=40,
        name="forward_last" if last else "forward_first",
    )(blocks, *weights)


def backward(blocks_ref, p_hbm, wo, wi, out_ref, blocks_hbm, p, g, e, sems):
    units, width = wo.shape
    copies = Copies(sems)
    slopes = copies.start(p_hbm, p)
    handed = copies.start(blocks_ref, blocks_hbm)
    keep_parts(g, load_blocks(blocks_ref, 0, width // 2))
    for k, c in enumerate(blocks_of(units)):
        back = dot3(cut(g), parts(wo[c, :]), 1, 1)
        if k == 0:
            wait(slopes)
        keep_parts(e, p[:, c] * back, columns=c)
    for at, left, right in output_columns(width):
        store_pair(out_ref, at, *(dot3(cut(e), parts(wi[c, :]), 1, 1) for c in (left, right)))
    wait(handed)


def run_backward(blocks, p, wo, wi):
    chips, _, lanes = blocks.shape
    units, width = wo.shape
    rows = chips * 4
    return call(
        backward,
        (struct(chips, 8, lanes), struct(chips, 8, lanes)),
        ins=[here, there, here, here],
        outs=(here, there),
        scratch=[
            pltpu.VMEM((rows, units), f32),
            pltpu.VMEM(tiled(rows, width), bf16),
            pltpu.VMEM(tiled(rows, units), bf16),
            pltpu.SemaphoreType.DMA((2,)),
        ],
        flops=2 * rows * width * units * 6,
        moved=8 * width * units,
        limit=12,
        name="backward_last",
    )(blocks, p, wo, wi)


def finish(blocks_hbm, p_hbm, wo_hbm, at_hbm, nt_hbm, in_hbm, out_hbm, *scratch):
    blocks, p, wo, at, nt, g, e, of_in, of_out, sems = scratch
    units, width = p.shape[1], nt.shape[2]
    sets = [[(blocks_hbm, blocks)], [(at_hbm, at)], [(wo_hbm, wo), (p_hbm, p)], [(nt_hbm, nt)]]
    copies = Copies(sems, sets)
    copies.begin(2)
    copies.wait(0, 1)
    copies.begin(4)
    keep_parts(g, load_blocks(blocks, 0, width // 2))
    results = []

    def put(source, target, rows):
        step = UNITS // PIECES
        for first in range(rows.start, rows.stop, step):
            some = slice(first, first + step)
            results.append(copies.start(source.at[some, :], target.at[some, :]))

    copies.wait(1, 2)
    for c in blocks_of(units):
        of_out[c, :] = dot3(cut(at, rows=c), cut(g))
        put(of_out, out_hbm, c)
    copies.wait(2, 4)
    for c in blocks_of(units):
        keep_parts(e, p[:, c] * dot3(cut(g), parts(wo[c, :]), 1, 1), columns=c)
    for c in blocks_of(width):
        of_in[c, :] = dot3(cut(nt, rows=c), cut(e))
        put(of_in, in_hbm, c)
    wait(*results)


def run_finish(blocks, p, wo, at, nt):
    units, width = at.shape[2], nt.shape[2]
    rows = at.shape[1] * LANES
    return call(
        finish,
        (struct(width, units), struct(units, width)),
        ins=[there] * 5,
        outs=(there, there),
        scratch=[
            pltpu.VMEM(blocks.shape, f32),
            pltpu.VMEM((rows, units), f32),
            pltpu.VMEM((units, width), f32),
            pltpu.VMEM(tiled(units, rows), bf16),
            pltpu.VMEM(tiled(width, rows), bf16),
            pltpu.VMEM(tiled(rows, width), bf16),
            pltpu.VMEM(tiled(rows, units), bf16),
            pltpu.VMEM((width, units), f32),
            pltpu.VMEM((units, width), f32),
            pltpu.SemaphoreType.DMA((5 + PIECES * (units + width) // UNITS,)),
        ],
        flops=2 * rows * width * units * 9,
        moved=12 * width * units,
        limit=36,
        name="finish",
    )(blocks, p, wo, at, nt)


def exchanged(blocks):
    return lax.all_to_all(blocks, "mp", 0, 0, tiled=True)


def on_device(tokens, curvature, gains, w_in, w_out, v_in, v_out):
    first = lax.axis_index("segment") == 0
    gain = gains
    weights = w_in[0], v_in[0], w_out[0], v_out[0]
    width = tokens.shape[2]
    rows = tokens.shape[0] * tokens.shape[1]
    chips = lax.axis_size("mp")
    total = rows * chips
    units = w_in.shape[2]
    single = struct(chips, 8, width // 2)
    double = struct(chips, 8, width)

    def blank(*shape, dtype=f32):
        return jnp.zeros(shape, dtype)

    def forward_first():
        blocks = exchanged(call(spread_first, single, name="spread_first")(tokens, gain))
        inward = run_split(*weights[:2])
        out, n, a, p = run_forward(blocks, (*inward, *weights[2:]), False)
        both = call(sum_first, struct(rows, 2 * width), name="sum_first")(exchanged(out), tokens)
        return both, n, a, p, inward

    def no_forward():
        return (
            blank(rows, 2 * width),
            blank(*tiled(total, width), dtype=bf16),
            blank(*tiled(total, units), dtype=bf16),
            blank(total, units),
            run_split(*weights[:2]),
        )

    both, n0, a0, p0, inward = lax.cond(first, forward_first, no_forward)
    both = lax.ppermute(both, "segment", [(0, 1)])

    def layer_last(both, n0, a0, p0, inward):
        blocks = exchanged(call(spread_last, double, name="spread_last")(both, gain))
        out, n, a, p = run_forward(blocks, (*inward, *weights[2:]), True)
        g, blocks = call(sum_last, (struct(rows, width), single), name="sum_last")(
            exchanged(out), both, curvature
        )
        out, blocks = run_backward(exchanged(blocks), p, weights[2], weights[0])
        back = call(sum_back, struct(rows, width), name="sum_back")(exchanged(out), g, both, gain)
        return back, blocks, p, *run_turn(n, a)

    def keep(both, n0, a0, p0, inward):
        return blank(rows, width), blank(*single.shape), p0, *run_turn(n0, a0)

    back, blocks, p, nt, at = lax.cond(first, keep, layer_last, both, n0, a0, p0, inward)
    back = lax.ppermute(back, "segment", [(1, 0)])

    def cotangent_first(back, blocks):
        return exchanged(call(spread, single, name="spread")(back))

    def pass_on(back, blocks):
        return blocks

    blocks = lax.cond(first, cotangent_first, pass_on, back, blocks)

    product_in, product_out = run_finish(blocks, p, weights[2], at, nt)
    return product_in[None], product_out[None]


def solution(mesh):
    rows = P(None, "mp", None)
    layer_in = P("segment", None, "mp")
    layer_out = P("segment", "mp", None)
    return jax.shard_map(
        on_device,
        mesh=mesh,
        in_specs=(rows, rows, P("segment", None), layer_in, layer_out, layer_in, layer_out),
        out_specs=(layer_in, layer_out),
        check_vma=False,
    )
```

```python
import functools

import jax
import jax.numpy as jnp
from jax import lax
from jax.experimental import pallas as pl
from jax.experimental.pallas import tpu as pltpu
from jax.sharding import PartitionSpec as P

eps = 1e-06
coeff = 0.7978845608028654
f32 = jnp.float32
bf16 = jnp.bfloat16
UNITS = 256
MIB = 1 << 20
LANES = 128
GROUP = 4
PIECES = 2
COVER_FLOPS = 1 << 34


def gelu_pair(h):
    inner = coeff * (h + 0.044715 * h * h * h)
    tval = jnp.tanh(inner)
    act = 0.5 * h * (1.0 + tval)
    slope = 0.5 * (1.0 + tval) + 0.5 * h * (1.0 - tval * tval) * coeff * (
        1.0 + 3.0 * 0.044715 * h * h
    )
    return act, slope


def mean(v):
    return jnp.mean(v, axis=-1, keepdims=True)


def parts(v):
    high = v.astype(bf16)
    return high, (v - high.astype(f32)).astype(bf16)


def dot3(a, b, ca=1, cb=0):
    dims = (((ca,), (cb,)), ((), ()))

    def one(x, y):
        return lax.dot_general(x, y, dims, preferred_element_type=f32)

    return one(a[0], b[0]) + one(a[1], b[0]) + one(a[0], b[1])


def to_block(rows):
    half = rows.shape[1] // 2
    return jnp.concatenate([rows[:, :half], rows[:, half:]], axis=0)


def from_block(block):
    rows = block.shape[0] // 2
    return jnp.concatenate([block[:rows], block[rows:]], axis=1)


def swap_halves(left, right):
    top = lax.broadcasted_iota(jnp.int32, left.shape, 1) < 4
    return (
        jnp.where(top, left, pltpu.roll(right, 4, 1)),
        jnp.where(top, pltpu.roll(left, 4, 1), right),
    )


def load_blocks(ref, at, half):
    blocks = ref[:, :, at : at + half]
    pairs = blocks.reshape(blocks.shape[0] // 2, 2, 8, half)
    left, right = swap_halves(pairs[:, 0], pairs[:, 1])
    whole = jnp.concatenate([left, right], axis=2)
    return whole.reshape(whole.shape[0] * 8, 2 * half)


def call(body, out, grid=None, ins=None, outs=None, scratch=(), flops=0, moved=0, limit=12, name=None):
    kwargs = {}
    if grid is not None:
        kwargs["grid"] = grid
    if ins is not None:
        kwargs.update(in_specs=ins, out_specs=outs)
    return pl.pallas_call(
        body,
        out_shape=out,
        scratch_shapes=list(scratch),
        compiler_params=pltpu.CompilerParams(vmem_limit_bytes=limit * MIB),
        cost_estimate=pl.CostEstimate(flops=flops, bytes_accessed=moved, transcendentals=0),
        name=name,
        **kwargs,
    )


here = pl.BlockSpec(memory_space=pltpu.VMEM)
there = pl.BlockSpec(memory_space=pl.ANY)


def struct(*shape, dtype=f32):
    return jax.ShapeDtypeStruct(shape, dtype)


def flat(ref):
    return jnp.concatenate([ref[0], ref[1]], axis=0)


def spread_first(tok_ref, gain_ref, out_ref):
    x = flat(tok_ref)
    n = x * lax.rsqrt(mean(x * x) + eps) * gain_ref[...]
    out_ref[...] = jnp.broadcast_to(to_block(n), out_ref.shape)


def spread(row_ref, out_ref):
    out_ref[...] = jnp.broadcast_to(to_block(row_ref[...]), out_ref.shape)


def spread_last(row_ref, gain_ref, out_ref):
    width = gain_ref.shape[1]
    x = row_ref[:, :width]
    dx = row_ref[:, width:]
    r = lax.rsqrt(mean(x * x) + eps)
    n = x * r * gain_ref[...]
    dn = gain_ref[...] * (dx * r - x * r**3 * mean(x * dx))
    half = width // 2
    out_ref[:, :, :half] = jnp.broadcast_to(to_block(n), (out_ref.shape[0], 8, half))
    out_ref[:, :, half:] = jnp.broadcast_to(to_block(dn), (out_ref.shape[0], 8, half))


def sum_first(blocks_ref, tok_ref, out_ref):
    total = jnp.sum(blocks_ref[...], axis=0)
    half = total.shape[1] // 2
    width = tok_ref.shape[2]
    out_ref[:, :width] = flat(tok_ref) + from_block(total[:, :half])
    out_ref[:, width:] = from_block(total[:, half:])


def sum_last(blocks_ref, row_ref, curv_ref, rows_ref, out_ref):
    width = curv_ref.shape[2]
    g = flat(curv_ref) * (row_ref[:, width:] + from_block(jnp.sum(blocks_ref[...], axis=0)))
    rows_ref[...] = g
    out_ref[...] = jnp.broadcast_to(to_block(g), out_ref.shape)


def sum_back(blocks_ref, g_ref, row_ref, gain_ref, out_ref):
    width = gain_ref.shape[1]
    u = gain_ref[...] * from_block(jnp.sum(blocks_ref[...], axis=0))
    x = row_ref[:, :width]
    r = lax.rsqrt(mean(x * x) + eps)
    out_ref[...] = g_ref[...] + u * r - x * r**3 * mean(x * u)


def split(*refs):
    half = len(refs) // 2
    for in_ref, out_ref in zip(refs[:half], refs[half:]):
        keep_parts(out_ref, in_ref[...])


def run_split(*weights):
    rows, columns = weights[0].shape
    step = 256
    count = len(weights)
    return call(
        split,
        (struct(*tiled(rows, columns), dtype=bf16),) * count,
        grid=(rows // step,),
        ins=[pl.BlockSpec((step, columns), lambda j: (j, 0))] * count,
        outs=(pl.BlockSpec(tiled(step, columns), lambda j: (0, 0, j, 0)),) * count,
        flops=COVER_FLOPS,
        moved=8 * rows * columns * count,
        limit=26,
        name="split",
    )(*weights)


def turn(n_ref, a_ref, nt_ref, at_ref):
    for ref, turned in ((n_ref, nt_ref), (a_ref, at_ref)):
        for b in range(ref.shape[1]):
            for k in range(2):
                t = ref[k, b].T
                for c in range(turned.shape[1]):
                    turned[k, c, b * LANES : (b + 1) * LANES, :] = t[:, c * LANES : (c + 1) * LANES]


def run_turn(n, a):
    return call(
        turn,
        tuple(struct(*tiled(v.shape[1] * LANES, v.shape[2]), dtype=bf16) for v in (n, a)),
        flops=COVER_FLOPS,
        moved=4 * (n.size + a.size),
        limit=12,
        name="turn",
    )(n, a)


def tiled(rows, columns):
    return 2, columns // LANES, rows, LANES


def groups(ref, columns):
    first, last = (0, ref.shape[1] * LANES) if columns is None else (columns.start, columns.stop)
    return slice(first // LANES, last // LANES)


def cut(ref, rows=slice(None), columns=None):
    some = groups(ref, columns)
    return tuple(
        jnp.concatenate([ref[k, b, rows, :] for b in range(some.start, some.stop)], axis=1) for k in range(2)
    )


def keep_parts(ref, value, rows=slice(None), columns=None):
    some = groups(ref, columns)
    for k, part in enumerate(parts(value)):
        for at, b in enumerate(range(some.start, some.stop)):
            ref[k, b, rows, :] = part[:, at * LANES : (at + 1) * LANES]


def blocks_of(size):
    return [slice(at, at + UNITS) for at in range(0, size, UNITS)]


def output_columns(width):
    half = width // 2
    return [(at, slice(at, at + UNITS), slice(half + at, half + at + UNITS)) for at in range(0, half, UNITS)]


def store_pair(out_ref, at, left, right):
    rows, lanes = left.shape
    even, odd = swap_halves(left.reshape(rows // 8, 8, lanes), right.reshape(rows // 8, 8, lanes))
    out_ref[:, :, at : at + lanes] = jnp.stack([even, odd], axis=1).reshape(rows // 4, 8, lanes)


class Copies:
    def __init__(self, sems, sets=()):
        self.sems = sems
        self.count = 0
        self.sets = list(sets)
        self.begun = []

    def start(self, source, target):
        copy = pltpu.make_async_copy(source, target, self.sems.at[self.count])
        self.count += 1
        copy.start()
        return copy

    def begin(self, upto):
        for pairs in self.sets[len(self.begun) : upto]:
            self.begun.append([self.start(*pair) for pair in pairs])

    def wait(self, first, last):
        self.begin(last)
        for begun in self.begun[first:last]:
            wait(*begun)


def wait(*copies):
    for copy in copies:
        copy.wait()


def forward(last, blocks_ref, wi_hbm, vi_hbm, wo_hbm, vo_hbm, out_ref, n_hbm, a_hbm, p_hbm, *scratch):
    wi, vi, wo, vo, n, a, p, da, d, sems = scratch
    units, width = wo.shape
    half = width // 2

    def some(source, target, cols):
        if len(source.shape) == 2:
            return source.at[:, cols], target.at[:, cols]
        return source.at[:, groups(source, cols)], target.at[:, groups(target, cols)]

    inward = [[some(wi_hbm, wi, c), some(vi_hbm, vi, c)] for c in blocks_of(units)]
    outward = [[some(wo_hbm, wo, c)] for _, *both in output_columns(width) for c in both]
    if last:
        vo = vo_hbm
    else:
        for k, c in enumerate(c for _, *both in output_columns(width) for c in both):
            outward[k].append(some(vo_hbm, vo, c))
    copies = Copies(sems, inward + outward)
    copies.begin(GROUP)
    keep_parts(n, load_blocks(blocks_ref, 0, half))
    if last:
        keep_parts(d, load_blocks(blocks_ref, half, half))
    for k, cols in enumerate(blocks_of(units)):
        if k % GROUP == 0:
            copies.wait(k, k + GROUP)
            copies.begin(k + 3 * GROUP)
        h = dot3(cut(n), cut(wi, columns=cols))
        dh = dot3(cut(n), cut(vi, columns=cols))
        if last:
            dh = dh + dot3(cut(d), cut(wi, columns=cols))
        act, slope = gelu_pair(h)
        p[:, cols] = slope
        keep_parts(a, act, columns=cols)
        keep_parts(da, slope * dh, columns=cols)
    results = [copies.start(n, n_hbm), copies.start(a, a_hbm), copies.start(p, p_hbm)]
    copies.wait(len(inward), len(copies.sets))
    for at, left, right in output_columns(width):
        wo_here = [parts(wo[:, c]) for c in (left, right)]
        if not last:
            store_pair(out_ref, at, *(dot3(cut(a), w) for w in wo_here))
        terms = [
            dot3(cut(da), w) + dot3(cut(a), parts(vo[:, c])) for w, c in zip(wo_here, (left, right))
        ]
        store_pair(out_ref, at + (0 if last else half), *terms)
    wait(*results)


def run_forward(blocks, weights, last):
    chips, _, lanes = blocks.shape
    units, width = weights[2].shape
    rows = chips * 4
    out_lanes = (1 if last else 2) * width // 2
    inward = pltpu.VMEM(tiled(width, units), bf16)
    outward = pltpu.VMEM((units, width), f32)
    small = pltpu.VMEM(tiled(rows, width), bf16)
    wide = pltpu.VMEM(tiled(rows, units), bf16)
    copies = 2 * (units // UNITS) + 2 * (width // UNITS) + 3
    return call(
        functools.partial(forward, last),
        (
            struct(chips, 8, out_lanes),
            struct(*tiled(rows, width), dtype=bf16),
            struct(*tiled(rows, units), dtype=bf16),
            struct(rows, units),
        ),
        ins=[here] + [there] * 3 + [here if last else there],
        outs=(here,) + (there,) * 3,
        scratch=[inward, inward, outward, pltpu.VMEM((8, 128), f32) if last else outward, small, wide, pltpu.VMEM((rows, units), f32), wide]
        + [small if last else pltpu.VMEM((8, 128), bf16), pltpu.SemaphoreType.DMA((copies,))],
        flops=2 * rows * width * units * 5 * 3,
        moved=4 * width * units * 4,
        limit=40,
        name="forward_last" if last else "forward_first",
    )(blocks, *weights)


def backward(blocks_ref, p_hbm, wo, wi, out_ref, blocks_hbm, p, g, e, sems):
    units, width = wo.shape
    copies = Copies(sems)
    slopes = copies.start(p_hbm, p)
    handed = copies.start(blocks_ref, blocks_hbm)
    keep_parts(g, load_blocks(blocks_ref, 0, width // 2))
    for k, c in enumerate(blocks_of(units)):
        back = dot3(cut(g), parts(wo[c, :]), 1, 1)
        if k == 0:
            wait(slopes)
        keep_parts(e, p[:, c] * back, columns=c)
    for at, left, right in output_columns(width):
        store_pair(out_ref, at, *(dot3(cut(e), parts(wi[c, :]), 1, 1) for c in (left, right)))
    wait(handed)


def run_backward(blocks, p, wo, wi):
    chips, _, lanes = blocks.shape
    units, width = wo.shape
    rows = chips * 4
    return call(
        backward,
        (struct(chips, 8, lanes), struct(chips, 8, lanes)),
        ins=[here, there, here, here],
        outs=(here, there),
        scratch=[
            pltpu.VMEM((rows, units), f32),
            pltpu.VMEM(tiled(rows, width), bf16),
            pltpu.VMEM(tiled(rows, units), bf16),
            pltpu.SemaphoreType.DMA((2,)),
        ],
        flops=2 * rows * width * units * 6,
        moved=8 * width * units,
        limit=12,
        name="backward_last",
    )(blocks, p, wo, wi)


def finish(blocks_hbm, p_hbm, wo_hbm, at_hbm, nt_hbm, in_hbm, out_hbm, *scratch):
    blocks, p, wo, at, nt, g, e, of_in, of_out, sems = scratch
    units, width = p.shape[1], nt.shape[2]
    sets = [[(blocks_hbm, blocks)], [(at_hbm, at)], [(wo_hbm, wo), (p_hbm, p)], [(nt_hbm, nt)]]
    copies = Copies(sems, sets)
    copies.begin(2)
    copies.wait(0, 1)
    copies.begin(4)
    keep_parts(g, load_blocks(blocks, 0, width // 2))
    results = []

    def put(source, target, rows):
        step = UNITS // PIECES
        for first in range(rows.start, rows.stop, step):
            some = slice(first, first + step)
            results.append(copies.start(source.at[some, :], target.at[some, :]))

    copies.wait(1, 2)
    for c in blocks_of(units):
        of_out[c, :] = dot3(cut(at, rows=c), cut(g))
        put(of_out, out_hbm, c)
    copies.wait(2, 4)
    for c in blocks_of(units):
        keep_parts(e, p[:, c] * dot3(cut(g), parts(wo[c, :]), 1, 1), columns=c)
    for c in blocks_of(width):
        of_in[c, :] = dot3(cut(nt, rows=c), cut(e))
        put(of_in, in_hbm, c)
    wait(*results)


def run_finish(blocks, p, wo, at, nt):
    units, width = at.shape[2], nt.shape[2]
    rows = at.shape[1] * LANES
    return call(
        finish,
        (struct(width, units), struct(units, width)),
        ins=[there] * 5,
        outs=(there, there),
        scratch=[
            pltpu.VMEM(blocks.shape, f32),
            pltpu.VMEM((rows, units), f32),
            pltpu.VMEM((units, width), f32),
            pltpu.VMEM(tiled(units, rows), bf16),
            pltpu.VMEM(tiled(width, rows), bf16),
            pltpu.VMEM(tiled(rows, width), bf16),
            pltpu.VMEM(tiled(rows, units), bf16),
            pltpu.VMEM((width, units), f32),
            pltpu.VMEM((units, width), f32),
            pltpu.SemaphoreType.DMA((5 + PIECES * (units + width) // UNITS,)),
        ],
        flops=2 * rows * width * units * 9,
        moved=12 * width * units,
        limit=36,
        name="finish",
    )(blocks, p, wo, at, nt)


def exchanged(blocks):
    return lax.all_to_all(blocks, "mp", 0, 0, tiled=True)


def on_device(tokens, curvature, gains, w_in, w_out, v_in, v_out):
    first = lax.axis_index("segment") == 0
    gain = gains
    weights = w_in[0], v_in[0], w_out[0], v_out[0]
    width = tokens.shape[2]
    rows = tokens.shape[0] * tokens.shape[1]
    chips = lax.axis_size("mp")
    total = rows * chips
    units = w_in.shape[2]
    single = struct(chips, 8, width // 2)
    double = struct(chips, 8, width)

    def blank(*shape, dtype=f32):
        return jnp.zeros(shape, dtype)

    def forward_first():
        blocks = exchanged(call(spread_first, single, name="spread_first")(tokens, gain))
        inward = run_split(*weights[:2])
        out, n, a, p = run_forward(blocks, (*inward, *weights[2:]), False)
        both = call(sum_first, struct(rows, 2 * width), name="sum_first")(exchanged(out), tokens)
        return both, n, a, p, inward

    def no_forward():
        return (
            blank(rows, 2 * width),
            blank(*tiled(total, width), dtype=bf16),
            blank(*tiled(total, units), dtype=bf16),
            blank(total, units),
            run_split(*weights[:2]),
        )

    both, n0, a0, p0, inward = lax.cond(first, forward_first, no_forward)
    both = lax.ppermute(both, "segment", [(0, 1)])

    def layer_last(both, n0, a0, p0, inward):
        blocks = exchanged(call(spread_last, double, name="spread_last")(both, gain))
        out, n, a, p = run_forward(blocks, (*inward, *weights[2:]), True)
        g, blocks = call(sum_last, (struct(rows, width), single), name="sum_last")(
            exchanged(out), both, curvature
        )
        out, blocks = run_backward(exchanged(blocks), p, weights[2], weights[0])
        back = call(sum_back, struct(rows, width), name="sum_back")(exchanged(out), g, both, gain)
        return back, blocks, p, *run_turn(n, a)

    def keep(both, n0, a0, p0, inward):
        return blank(rows, width), blank(*single.shape), p0, *run_turn(n0, a0)

    back, blocks, p, nt, at = lax.cond(first, keep, layer_last, both, n0, a0, p0, inward)
    back = lax.ppermute(back, "segment", [(1, 0)])

    def cotangent_first(back, blocks):
        return exchanged(call(spread, single, name="spread")(back))

    def pass_on(back, blocks):
        return blocks

    blocks = lax.cond(first, cotangent_first, pass_on, back, blocks)

    product_in, product_out = run_finish(blocks, p, weights[2], at, nt)
    return product_in[None], product_out[None]


def solution(mesh):
    rows = P(None, "mp", None)
    layer_in = P("segment", None, "mp")
    layer_out = P("segment", "mp", None)
    return jax.shard_map(
        on_device,
        mesh=mesh,
        in_specs=(rows, rows, P("segment", None), layer_in, layer_out, layer_in, layer_out),
        out_specs=(layer_in, layer_out),
        check_vma=False,
    )
```
